32 devices in a mesh: gx: 2 (over x), gy: 4 (over y, core), gz: 4 (over z).
Axes of the slice: x: 2, y: 2, z: 4, core: 2. Of those that a mesh axis runs over, the one named last changes fastest.
Arguments:
- panels: bfloat16 [3072, 8192], P(('gx', 'gy'), 'gz'), may hold values from -0.75 to 0.75
- sizes: int32 [8], replicated, may hold values from 1 to 1024
- front: float32 [3072, 3072], P(('gx', 'gz'), 'gy'), may hold values from -6 to 6
Outputs:
- updated: float32 [3072, 3072], P(('gx', 'gz'), 'gy')
The draws below stay inside these ranges and needn't reach their ends.
All inputs are finite; a program needn't handle non-finite values.
Results may differ from the reference program's by a relative error of at most 0.0003.
Values may be sent and summed in bfloat16 or wider, within the bound.
No kernel may reach another device: no remote copies, remote signals or barrier semaphores. Data moves between devices by JAX's collectives and lax.ppermute only.
A program may use at most 128 MiB of HBM per device.

```python
import jax
import jax.numpy as jnp

WIDTH = 1024
ROWS_PIECE = 384
HEIGHT = 3072
SUPER = 8
N_GX = 2
N_GY = 4


def place_ends(result, key, low, largest):
    shape = result.shape
    index_at = [jax.random.randint(jax.random.fold_in(key, axis), (), 0, shape[axis]) for axis in range(len(shape))]
    result = result.at[tuple(index_at)].set(low)
    longest = shape.index(max(shape))
    index_at[longest] = (index_at[longest] + 1) % shape[longest]
    return result.at[tuple(index_at)].set(largest)


def block_levels(rng, dims, pieces, low, top_value):
    factor_of, own = 1.0, jax.random.fold_in(rng, 6)
    for axis_at, parts in pieces:
        steps = jnp.exp(jax.random.uniform(jax.random.fold_in(own, axis_at), (parts,), jnp.float32, low / len(pieces), top_value / len(pieces)))
        factor_of = factor_of * jnp.repeat(steps, dims[axis_at] // parts).reshape([-1 if axis == axis_at else 1 for axis in range(len(dims))])
    return factor_of


def centred(rng, dims, scale, limit, cuts=(), held_as=jnp.bfloat16):
    values = jax.random.normal(rng, dims, jnp.float32) * scale
    if len(cuts) > 0:
        values = block_levels(rng, dims, cuts, -0.22, 0.18) * values
    return jnp.clip(values, min=-limit, max=limit).astype(held_as)


def setup_inputs(seed: int = 0) -> dict:
    keys = jax.random.split(jax.random.key(seed), 4)
    panels = centred(keys[0], (HEIGHT, SUPER * WIDTH), 0.125, 0.75, ((0, 8), (1, 4)))
    sizes = place_ends(jax.random.randint(keys[1], (SUPER,), 1, WIDTH + 1), jax.random.fold_in(keys[1], 1), 1, WIDTH).astype(jnp.int32)
    front = centred(keys[2], (HEIGHT, HEIGHT), 1.0, 6.0, ((0, 8), (1, 4)), jnp.float32)
    return {"panels": panels, "sizes": sizes, "front": front}


def reference(panels, sizes, front):
    column = jnp.arange(WIDTH, dtype=jnp.int32)
    live = (column[None, :] < sizes[:, None]).reshape(SUPER * WIDTH).astype(jnp.bfloat16)
    masked = panels * live[None, :]
    update = jnp.dot(masked, panels.T, preferred_element_type=jnp.float32)
    update = update.reshape(HEIGHT, N_GX, N_GY, ROWS_PIECE).transpose(0, 2, 1, 3).reshape(HEIGHT, HEIGHT)
    return front - update
```

```python
import functools

import jax
import jax.numpy as jnp
from jax import lax
from jax.experimental import pallas as pl
from jax.experimental.pallas import tpu as pltpu
from jax.sharding import PartitionSpec as P

WIDTH = 1024
GROUP = 64
CODES = 16
STEPS = 256.0
TOP = 32767.0


def plain(panels, sizes, front):
    piece_rows = panels.shape[0]
    panel_count = panels.shape[1] // WIDTH
    first = lax.axis_index("gz") * panel_count
    limits = lax.dynamic_slice_in_dim(sizes, first, panel_count, 0)
    column = jnp.arange(WIDTH, dtype=jnp.int32)
    live = (column[None, :] < limits[:, None]).reshape(panel_count * WIDTH).astype(jnp.bfloat16)
    gathered = lax.all_gather(panels, ("gx", "gy"), axis=0, tiled=True)
    count_x = lax.axis_size("gx")
    count_y = lax.axis_size("gy")
    block_rows = piece_rows * count_y
    row_part = lax.dynamic_slice_in_dim(gathered, lax.axis_index("gx") * block_rows, block_rows, 0)
    grouped = gathered.reshape(count_x, count_y, piece_rows, panels.shape[1])
    column_part = lax.dynamic_index_in_dim(grouped, lax.axis_index("gy"), 1, keepdims=False)
    column_part = column_part.reshape(count_x * piece_rows, panels.shape[1])
    masked = row_part * live[None, :]
    summed = lax.psum_scatter(
        -lax.dot_general(
            masked, column_part, (((1,), (1,)), ((), ())), preferred_element_type=jnp.float32
        ),
        "gz",
        scatter_dimension=0,
        tiled=True,
    )
    return front + summed


def place(rnd, n):
    g = lax.axis_index("gy")
    z = lax.axis_index("gz")
    own_half = g // (n // 2)
    half = own_half if rnd == 0 else 1 - own_half
    w = jnp.where(half == 1, z, n - 1 - z)
    far = jnp.where(half == 1, n - 1, 0)
    return g, z, w, far


def choice(rnd, kind, n):
    g, _, _, far = place(rnd, n)
    if rnd == 0:
        first = (g == far) if kind == "far" else (g != far)
    else:
        inner = (g == 1) | (g == 2)
        first = inner if kind == "far" else jnp.logical_not(inner)
    return jnp.where(first, 0, 1)


def live_row(limits_ref, z, width):
    count = width // WIDTH
    column = lax.broadcasted_iota(jnp.int32, (1, WIDTH), 1)
    parts = [(column < limits_ref[z * count + p]).astype(jnp.float32) for p in range(count)]
    row = parts[0] if count == 1 else jnp.concatenate(parts, axis=1)
    return row.astype(jnp.bfloat16)


def product(rows_ref, cols_ref, live):
    return lax.dot_general(
        rows_ref[...] * live, cols_ref[...], (((1,), (1,)), ((), ())), preferred_element_type=jnp.float32
    )


def decode(packet_ref, rows, group, codes):
    scale = jnp.exp2(codes[group : group + 1, :] * (1.0 / STEPS)) * (1.0 / TOP)
    values = packet_ref[group * rows : (group + 1) * rows, :].astype(jnp.int32).astype(jnp.float32)
    return values * scale


def read_codes(packet_ref, height):
    return packet_ref[height : height + CODES, :].astype(jnp.int32).astype(jnp.float32)


def step_kernel(rnd, kind, step, n, limits_ref, rows0, rows1, cols, *rest):
    has_prev = step > 0
    if has_prev:
        prev, out_ref, rows_v, cols_v, prev_v, total, sems = rest
    else:
        out_ref, rows_v, cols_v, total, sems = rest
    g, z, w, far = place(rnd, n)
    active = w == step
    if kind == "near" and step == 0:
        active = active | (w == n - 1)
    which = choice(rnd, kind, n)

    @pl.when(active)
    def _():
        col_copy = pltpu.make_async_copy(cols, cols_v, sems.at[1])
        col_copy.start()
        if has_prev:
            prev_copy = pltpu.make_async_copy(prev, prev_v, sems.at[2])
            prev_copy.start()

        @pl.when(which == 0)
        def _():
            pltpu.make_async_copy(rows0, rows_v, sems.at[0]).start()

        @pl.when(which == 1)
        def _():
            pltpu.make_async_copy(rows1, rows_v, sems.at[0]).start()

        live = live_row(limits_ref, z, rows_v.shape[1])
        pltpu.make_async_copy(rows0, rows_v, sems.at[0]).wait()
        col_copy.wait()
        total[...] = product(rows_v, cols_v, live)
        if has_prev:
            prev_copy.wait()
            held = read_codes(prev_v, total.shape[0])
        height, width = total.shape
        line = lax.broadcasted_iota(jnp.int32, (CODES, width), 0)
        codes = jnp.zeros((CODES, width), jnp.float32)
        for group in range(height // GROUP):
            part = total[group * GROUP : (group + 1) * GROUP, :]
            if has_prev:
                part = part + decode(prev_v, GROUP, group, held)
            most = jnp.max(jnp.abs(part), axis=0, keepdims=True)
            code = jnp.ceil(jnp.log2(jnp.maximum(most, 1e-30)) * STEPS) + 1.0
            scaled = jnp.round(part * (jnp.exp2(code * (-1.0 / STEPS)) * TOP))
            scaled = jnp.clip(scaled, -TOP, TOP)
            out_ref[group * GROUP : (group + 1) * GROUP, :] = scaled.astype(jnp.int32).astype(jnp.int16)
            codes = jnp.where(line == group, code, codes)
        out_ref[height : height + CODES, :] = codes.astype(jnp.int32).astype(jnp.int16)


HBM = pl.BlockSpec(memory_space=pltpu.HBM)
VMEM = pl.BlockSpec(memory_space=pltpu.VMEM)
SMEM = pl.BlockSpec(memory_space=pltpu.SMEM)


def step_call(rnd, kind, step, n, sizes, pair, cols, prev):
    rows, width = cols.shape
    scratch = [pltpu.VMEM((rows, width), jnp.bfloat16), pltpu.VMEM((rows, width), jnp.bfloat16)]
    if prev is not None:
        scratch.append(pltpu.VMEM((rows + CODES, rows), jnp.int16))
    scratch += [pltpu.VMEM((rows, rows), jnp.float32), pltpu.SemaphoreType.DMA((3,))]
    operands = [sizes, pair[0], pair[1], cols] + ([prev] if prev is not None else [])
    return pl.pallas_call(
        functools.partial(step_kernel, rnd, kind, step, n),
        out_shape=jax.ShapeDtypeStruct((rows + CODES, rows), jnp.int16),
        in_specs=[SMEM] + [HBM] * (len(operands) - 1),
        out_specs=VMEM,
        scratch_shapes=scratch,
        cost_estimate=pl.CostEstimate(
            flops=2 * rows * rows * width, bytes_accessed=6 * rows * width, transcendentals=0
        ),
        name=f"step_{rnd}_{kind}_{step}",
    )(*operands)


def base_kernel(n, count_x, limits_ref, front, r00, r01, f0, f1, n0, n1, *rest):
    cols = rest[:count_x]
    out_ref, rows_v, cols_v, front_v, sems = rest[count_x:]
    g, z, _, _ = place(0, n)
    x = lax.axis_index("gx")
    mine = (z // (n // 2)) == (g // (n // 2))
    edge = (z == 0) | (z == n - 1)
    inner = (g == 1) | (g == 2)
    at = jnp.where(
        mine,
        jnp.where(z == g, 0, 1),
        jnp.where(edge, jnp.where(inner, 2, 3), jnp.where(inner, 5, 4)),
    )
    copies = [pltpu.make_async_copy(front, front_v, sems.at[1])]
    for d in range(count_x):
        copies.append(pltpu.make_async_copy(cols[d], cols_v.at[d], sems.at[2 + d]))
    for copy in copies:
        copy.start()
    for index, source in enumerate((r00, r01, f0, f1, n0, n1)):

        @pl.when(at == index)
        def _(source=source):
            pltpu.make_async_copy(source, rows_v, sems.at[0]).start()

    live = live_row(limits_ref, z, rows_v.shape[1])
    pltpu.make_async_copy(r00, rows_v, sems.at[0]).wait()
    copies[0].wait()
    rows = rows_v.shape[0]
    for d in range(count_x):
        copies[1 + d].wait()
        at_column = pl.ds(pl.multiple_of(lax.rem(x + d, count_x) * rows, 128), rows)
        out_ref[:, at_column] = front_v[:, at_column] - product(rows_v, cols_v.at[d], live)


def final_kernel(n, count_x, base_ref, *rest):
    packets = rest[: 6 * count_x]
    out_ref, held, sems = rest[6 * count_x :]
    x = lax.axis_index("gx")
    rows = base_ref.shape[0]
    out_ref[...] = base_ref[...]

    def subtract(slot, at_column):
        codes = read_codes(held.at[slot], rows)
        for group in range(rows // GROUP):
            at_row = slice(group * GROUP, (group + 1) * GROUP)
            out_ref[at_row, at_column] -= decode(held.at[slot], GROUP, group, codes)

    for rnd in range(2):
        _, _, w, _ = place(rnd, n)

        @pl.when(w == n - 1)
        def _(rnd=rnd, w=w):
            copies = []
            for d in range(count_x):
                copy = pltpu.make_async_copy(packets[6 * d + 3 * rnd + 2], held.at[2 * d], sems.at[2 * d])
                copy.start()
                copies.append(copy)
            for d in range(count_x):
                copies[d].wait()
                subtract(2 * d, pl.ds(pl.multiple_of(lax.rem(x + d, count_x) * rows, 128), rows))

        @pl.when(w == n - 2)
        def _(rnd=rnd, w=w):
            copies = []
            for d in range(count_x):
                for k in range(2):
                    copy = pltpu.make_async_copy(
                        packets[6 * d + 3 * rnd + k], held.at[2 * d + k], sems.at[2 * d + k]
                    )
                    copy.start()
                    copies.append(copy)
            for d in range(count_x):
                at_column = pl.ds(pl.multiple_of(lax.rem(x + d, count_x) * rows, 128), rows)
                for k in range(2):
                    copies[2 * d + k].wait()
                    subtract(2 * d + k, at_column)


def shards(n, count_x, panels, sizes, front):
    rows, width = panels.shape

    def along_y(value, pairs):
        return lax.ppermute(value, "gy", pairs)

    def along_z(value, rnd, hops):
        pairs = []
        for g in range(n):
            half = g // (n // 2) if rnd == 0 else 1 - g // (n // 2)
            for a, b in hops:
                source, target = (a, b) if half == 1 else (n - 1 - a, n - 1 - b)
                pairs.append((g * n + source, g * n + target))
        return lax.ppermute(value, ("gy", "gz"), pairs)

    beside = along_y(panels, [(g, g ^ 1) for g in range(n)])
    far_first = along_y(panels, [(0, 2), (3, 1)])
    cols = [panels] + [
        lax.ppermute(panels, "gx", [((i + d) % count_x, i) for i in range(count_x)]) for d in range(1, count_x)
    ]
    near_first = along_y(beside, [(0, 3), (3, 0)])
    far_second = along_y(far_first, [(2, 3), (1, 0)])
    near_second = along_y(near_first, [(3, 2), (0, 1)])
    pairs = {
        (0, "far"): (panels, beside),
        (0, "near"): (panels, beside),
        (1, "far"): (far_first, far_second),
        (1, "near"): (near_first, near_second),
    }

    packets = []
    for d in range(count_x):
        for rnd in range(2):
            near = far = None
            ends = []
            for step, hops in enumerate(([(0, 1), (n - 1, n - 2)], [(1, 2)])):
                near = along_z(step_call(rnd, "near", step, n, sizes, pairs[rnd, "near"], cols[d], near), rnd, hops)
                ends.append(near)
            for step in range(3):
                far = along_z(
                    step_call(rnd, "far", step, n, sizes, pairs[rnd, "far"], cols[d], far), rnd, [(step, step + 1)]
                )
            packets += ends + [far]

    base = pl.pallas_call(
        functools.partial(base_kernel, n, count_x),
        out_shape=jax.ShapeDtypeStruct(front.shape, jnp.float32),
        in_specs=[SMEM] + [HBM] * (7 + count_x),
        out_specs=VMEM,
        scratch_shapes=[
            pltpu.VMEM((rows, width), jnp.bfloat16),
            pltpu.VMEM((count_x, rows, width), jnp.bfloat16),
            pltpu.VMEM(front.shape, jnp.float32),
            pltpu.SemaphoreType.DMA((2 + count_x,)),
        ],
        cost_estimate=pl.CostEstimate(
            flops=2 * rows * rows * width * count_x, bytes_accessed=6 * rows * width, transcendentals=0
        ),
        name="base",
    )(sizes, front, panels, beside, far_first, far_second, near_first, near_second, *cols)
    return pl.pallas_call(
        functools.partial(final_kernel, n, count_x),
        out_shape=jax.ShapeDtypeStruct(front.shape, jnp.float32),
        in_specs=[VMEM] + [HBM] * (6 * count_x),
        out_specs=VMEM,
        scratch_shapes=[
            pltpu.VMEM((2 * count_x, rows + CODES, rows), jnp.int16),
            pltpu.SemaphoreType.DMA((2 * count_x,)),
        ],
        cost_estimate=pl.CostEstimate(flops=4 * rows * rows, bytes_accessed=12 * rows * rows, transcendentals=0),
        name="final",
    )(base, *packets)


def solution(mesh):
    n, count_x = mesh.shape["gz"], mesh.shape["gx"]
    in_specs = (P(("gx", "gy"), "gz"), P(), P(("gx", "gz"), "gy"))
    out_specs = P(("gx", "gz"), "gy")
    fits = n == 4 and mesh.shape["gy"] == n
    body = functools.partial(shards, n, count_x) if fits else plain
    return jax.shard_map(body, mesh=mesh, in_specs=in_specs, out_specs=out_specs, check_vma=False)
```

```python
import functools

import jax
import jax.numpy as jnp
from jax import lax
from jax.experimental import pallas as pl
from jax.experimental.pallas import tpu as pltpu
from jax.sharding import PartitionSpec as P


WIDTH = 1024
GROUP = 64
CODES = 16
STEPS = 256.0
TOP = 32767.0


def plain(panels, sizes, front):
    piece_rows = panels.shape[0]
    panel_count = panels.shape[1] // WIDTH
    first = lax.axis_index("gz") * panel_count
    limits = lax.dynamic_slice_in_dim(sizes, first, panel_count, 0)
    column = jnp.arange(WIDTH, dtype=jnp.int32)
    live = (column[None, :] < limits[:, None]).reshape(panel_count * WIDTH).astype(jnp.bfloat16)
    gathered = lax.all_gather(panels, ("gx", "gy"), axis=0, tiled=True)
    count_x = lax.axis_size("gx")
    count_y = lax.axis_size("gy")
    block_rows = piece_rows * count_y
    row_part = lax.dynamic_slice_in_dim(gathered, lax.axis_index("gx") * block_rows, block_rows, 0)
    grouped = gathered.reshape(count_x, count_y, piece_rows, panels.shape[1])
    column_part = lax.dynamic_index_in_dim(grouped, lax.axis_index("gy"), 1, keepdims=False)
    column_part = column_part.reshape(count_x * piece_rows, panels.shape[1])
    masked = row_part * live[None, :]
    summed = lax.psum_scatter(
        -lax.dot_general(
            masked, column_part, (((1,), (1,)), ((), ())), preferred_element_type=jnp.float32
        ),
        "gz",
        scatter_dimension=0,
        tiled=True,
    )
    return front + summed


def place(rnd, n):
    g = lax.axis_index("gy")
    z = lax.axis_index("gz")
    own_half = g // (n // 2)
    half = own_half if rnd == 0 else 1 - own_half
    w = jnp.where(half == 1, z, n - 1 - z)
    far = jnp.where(half == 1, n - 1, 0)
    return g, w, far


def product(rows, cols_ref, live_ref):
    return lax.dot_general(
        rows * live_ref[...], cols_ref[...], (((1,), (1,)), ((), ())), preferred_element_type=jnp.float32
    )


def decode(packet_ref, group, codes):
    scale = jnp.exp2(codes[group : group + 1, :] * (1.0 / STEPS)) * (1.0 / TOP)
    values = packet_ref[group * GROUP : (group + 1) * GROUP, :].astype(jnp.int32).astype(jnp.float32)
    return values * scale


def read_codes(packet_ref):
    height = packet_ref.shape[0] - CODES
    return packet_ref[height:, :].astype(jnp.int32).astype(jnp.float32)


def encode(out_ref, read):
    height, width = out_ref.shape[0] - CODES, out_ref.shape[1]
    line = lax.broadcasted_iota(jnp.int32, (CODES, width), 0)
    codes = jnp.zeros((CODES, width), jnp.float32)
    for group in range(height // GROUP):
        part = read(group)
        most = jnp.max(jnp.abs(part), axis=0, keepdims=True)
        code = jnp.ceil(jnp.log2(jnp.maximum(most, 1e-30)) * STEPS) + 1.0
        scaled = jnp.round(part * (jnp.exp2(code * (-1.0 / STEPS)) * TOP))
        scaled = jnp.clip(scaled, -TOP, TOP)
        out_ref[group * GROUP : (group + 1) * GROUP, :] = scaled.astype(jnp.int32).astype(jnp.int16)
        codes = jnp.where(line == group, code, codes)
    out_ref[height:, :] = codes.astype(jnp.int32).astype(jnp.int16)


def rows_of(group):
    return slice(group * GROUP, (group + 1) * GROUP)


def rows_of(group):
    return slice(group * GROUP, (group + 1) * GROUP)


def headed(to, n):
    g = lax.axis_index("gy")
    return jnp.where(g // (n // 2) == to // (n // 2), 0, 1)


def at_ends(n):
    g = lax.axis_index("gy")
    return (g == 0) | (g == n - 1)


def own_kernel(n, live, panels, beside, cols, sums, packet):
    g, w, far = place(0, n)
    sums[0] = product(panels[...], cols, live)
    sums[1] = product(beside[...], cols, live)
    at = jnp.where((g == far) == (w == 0), 0, 1)
    encode(packet, lambda group: sums[at, rows_of(group), :])


def own_step_kernel(step, n, sums, held, packet):
    g, w, far = place(0, n)

    @pl.when((w <= step) & (w >= step - 1))
    def _():
        codes = read_codes(held)
        at = jnp.where((g == far) == (w == step), 0, 1)
        encode(packet, lambda group: sums[at, rows_of(group), :] + decode(held, group, codes))


def other_kernel(kind, n, live, first, second, cols, sums, packet):
    pick = at_ends(n) == (kind == "near")
    sums[...] = product(jnp.where(pick, first[...], second[...]), cols, live)
    encode(packet, lambda group: sums[rows_of(group), :])


def other_step_kernel(step, n, sums, held, packet):
    _, w, _ = place(1, n)

    @pl.when(w == step)
    def _():
        codes = read_codes(held)
        encode(packet, lambda group: sums[rows_of(group), :] + decode(held, group, codes))


def both_kernel(kind, n, live, panels, beside, first, second, cols, sums, *packets):
    z = lax.axis_index("gz")
    ends = at_ends(n)
    near = kind == "near"
    top = n - 2 if near else n - 1
    sums[0] = product(jnp.where(ends != near, panels[...], beside[...]), cols, live)
    sums[1] = product(jnp.where(ends == near, first[...], second[...]), cols, live)
    for index, packet in enumerate(packets):

        @pl.when((z == 0) | (z == n - 1))
        def _(index=index, packet=packet):
            up = (z == 0) == (index == 0)
            at = jnp.where(up, headed(top, n), headed(n - 1 - top, n))
            encode(packet, lambda group: sums[at, rows_of(group), :])


def both_step_kernel(kind, step, n, sums, held, packet):
    z = lax.axis_index("gz")
    top = n - 2 if kind == "near" else n - 1

    @pl.when((z == step) | (z == n - 1 - step))
    def _():
        codes = read_codes(held)
        at = jnp.where(z == step, headed(top, n), headed(n - 1 - top, n))
        encode(packet, lambda group: sums[at, rows_of(group), :] + decode(held, group, codes))


VMEM = pl.BlockSpec(memory_space=pltpu.VMEM)


def call(kernel, outs, operands, flops):
    size = sum(v.size * v.dtype.itemsize for v in (*operands, *outs))
    return pl.pallas_call(
        kernel,
        out_shape=outs if len(outs) > 1 else outs[0],
        in_specs=[VMEM] * len(operands),
        out_specs=[VMEM] * len(outs) if len(outs) > 1 else VMEM,
        compiler_params=pltpu.CompilerParams(vmem_limit_bytes=min(size + (4 << 20), 60 << 20)),
        cost_estimate=pl.CostEstimate(flops=flops, bytes_accessed=size, transcendentals=0),
    )(*operands)


def base_kernel(n, count_x, front, *rest):
    sums, out_ref = rest[:-1], rest[-1]
    x = lax.axis_index("gx")
    z = lax.axis_index("gz")
    rows = front.shape[0]
    g, w, far = place(0, n)

    def columns(d):
        return pl.ds(pl.multiple_of(lax.rem(x + d, count_x) * rows, 128), rows)

    @pl.when(w >= n // 2)
    def _():
        at = jnp.where((g == far) == (w == n - 1), 0, 1)
        out_ref[:, columns(0)] = front[:, columns(0)] - sums[0][at]

    for at_w, index in ((0, 1), (1, 2)):

        @pl.when(w == at_w)
        def _(index=index):
            out_ref[:, columns(0)] = front[:, columns(0)] - sums[index][...]

    edge = (z == 0) | (z == n - 1)
    for d in range(1, count_x):
        for side, index in ((edge, 1 + 2 * d), (jnp.logical_not(edge), 2 + 2 * d)):

            @pl.when(side)
            def _(d=d, index=index):
                mine = jnp.where(w >= n // 2, 0, 1)
                out_ref[:, columns(d)] = front[:, columns(d)] - sums[index][mine]


def final_kernel(n, count_x, base, *rest):
    packets, out_ref = rest[:-1], rest[-1]
    x = lax.axis_index("gx")
    z = lax.axis_index("gz")
    rows = base.shape[0]
    _, w, _ = place(0, n)

    def finish(d, picks):
        columns = pl.ds(pl.multiple_of(lax.rem(x + d, count_x) * rows, 128), rows)
        refs = [packets[k] for k in picks]
        codes = [read_codes(ref) for ref in refs]
        for group in range(rows // GROUP):
            value = base[rows_of(group), columns]
            for ref, code in zip(refs, codes):
                value = value - decode(ref, group, code)
            out_ref[rows_of(group), columns] = value

    for at, picks in ((n - 1, (1,)), (n - 2, (0, 1)), (0, (2,)), (1, (3, 4))):

        @pl.when(w == at)
        def _(picks=picks):
            finish(0, picks)

    edge = (z == 0) | (z == n - 1)
    for d in range(1, count_x):
        for side, picks in ((edge, (2 + 3 * d,)), (jnp.logical_not(edge), (3 + 3 * d, 4 + 3 * d))):

            @pl.when(side)
            def _(d=d, picks=picks):
                finish(d, picks)


def plan(count_x):
    crossed = range(1, count_x)

    def go(label, step):
        return [f"{label}_k{step}", f">{label}_{step}"]

    names = [">beside", ">far0"] + [f">cross{d}" for d in crossed] + [">near0"]
    names += go("own", 0) + go("own", 1) + [">far1"] + go("far", 0) + go("own", 2)
    for d in crossed:
        names += go(f"xf{d}", 0)
    names += [">near1"] + go("far", 1)
    for d in crossed:
        names += go(f"xn{d}", 0)
    names += go("near", 0)
    for d in crossed:
        names += [f">xn{d}_x"]
    for d in crossed:
        names += go(f"xf{d}", 1)
    names += go("far", 2)
    for d in crossed:
        names += go(f"xn{d}", 1)
    for d in crossed:
        names += go(f"xf{d}", 2)
    return names + go("near", 1) + ["base", "final"]


def shards(n, count_x, panels, sizes, front):
    rows, width = panels.shape
    square = 2 * rows * rows * width
    sums1 = jax.ShapeDtypeStruct((rows, rows), jnp.float32)
    sums2 = jax.ShapeDtypeStruct((2, rows, rows), jnp.float32)
    packet = jax.ShapeDtypeStruct((rows + CODES, rows), jnp.int16)
    block = jax.ShapeDtypeStruct(front.shape, jnp.float32)

    def move(value, axes, pairs):
        return lax.ppermute(value, axes, pairs)

    def way(rnd, hops):
        pairs = []
        for g in range(n):
            half = g // (n // 2) if rnd == 0 else 1 - g // (n // 2)
            for a, b in hops:
                source, target = (a, b) if half == 1 else (n - 1 - a, n - 1 - b)
                pairs.append((g * n + source, g * n + target))
        return pairs

    def both(hop):
        return way(0, [hop]) + way(1, [hop])

    count = width // WIDTH
    here = jnp.arange(sizes.size, dtype=jnp.int32)[:, None] == lax.axis_index("gz") * count + jnp.arange(count)[None, :]
    limits = jnp.sum(jnp.where(here, sizes[:, None], 0), axis=0)
    live = (jnp.arange(WIDTH)[None, :] < limits[:, None]).reshape(1, width).astype(jnp.bfloat16)

    hops = {
        "own_0": way(0, [(0, 1), (n - 1, n - 2)]),
        "own_1": way(0, [(0, 1), (1, 2)]),
        "own_2": way(0, [(1, 2), (2, 3)]),
        "far_0": way(1, [(0, 1)]),
        "far_1": way(1, [(1, 2)]),
        "far_2": way(1, [(2, 3)]),
        "near_0": way(1, [(0, 1), (n - 1, n - 2)]),
        "near_1": way(1, [(1, 2)]),
        "xf_0": both((0, 1)),
        "xf_1": both((1, 2)),
        "xf_2": both((2, 3)),
        "xn_0": both((0, 1)),
        "xn_1": both((1, 2)),
        "xn_x": both((n - 1, n - 2)),
    }
    y_moves = {
        "beside": (None, [(g, g ^ 1) for g in range(n)]),
        "far0": (None, [(0, 2), (3, 1)]),
        "near0": ("beside", [(0, 3), (3, 0)]),
        "far1": ("far0", [(2, 3), (1, 0)]),
        "near1": ("near0", [(3, 2), (0, 1)]),
    }
    held = {}
    sums = {}
    sent = {}
    got = {}
    for name in plan(count_x):
        label = name.lstrip(">")
        part, _, step = label.partition("_")
        step = step.lstrip("k")
        kind, d = part.rstrip("0123456789"), int("0" + part.lstrip("abcdefghijklmnopqrstuvwxyz"))
        if label in y_moves:
            source, pairs = y_moves[label]
            held[label] = move(panels if source is None else held[source], "gy", pairs)
        elif kind == "cross":
            held[label] = move(panels, "gx", [((i + d) % count_x, i) for i in range(count_x)])
        elif name[0] == ">":
            got[label] = move(sent[label], ("gy", "gz"), hops[f"{kind}_{step}"])
        elif label == "base":
            each = [sums[k] for k in ("own", "far", "near")]
            each += [sums[f"{k}{d}"] for d in range(1, count_x) for k in ("xf", "xn")]
            base = call(functools.partial(base_kernel, n, count_x), [block], [front, *each], 1)
        elif label == "final":
            each = [got[k] for k in ("own_0", "own_2", "far_2", "near_0", "near_1")]
            for d in range(1, count_x):
                each += [got[f"xf{d}_2"], got[f"xn{d}_1"], got[f"xn{d}_x"]]
            return call(functools.partial(final_kernel, n, count_x), [block], [base, *each], 1)
        elif step == "0":
            cols = held[f"cross{d}"] if d else panels
            local = (panels, held["beside"])
            other = () if kind == "own" else (held["far0"], held["far1"])
            if kind in ("near", "xn"):
                other = (held["near0"], held["near1"])
            if kind == "own":
                kernel, pieces, outs = functools.partial(own_kernel, n), local, [sums2, packet]
            elif kind in ("far", "near"):
                kernel, pieces, outs = functools.partial(other_kernel, kind, n), other, [sums1, packet]
            else:
                kernel = functools.partial(both_kernel, "far" if kind == "xf" else "near", n)
                pieces, outs = (*local, *other), [sums2, packet] + [packet] * (kind == "xn")
            done = call(kernel, outs, [live, *pieces, cols], len(pieces) * square // 2)
            sums[part], sent[f"{part}_0"] = done[:2]
            sent[f"{part}_x"] = done[-1]
        else:
            kernel = {
                "own": functools.partial(own_step_kernel, int(step), n),
                "far": functools.partial(other_step_kernel, int(step), n),
                "near": functools.partial(other_step_kernel, int(step), n),
                "xf": functools.partial(both_step_kernel, "far", int(step), n),
                "xn": functools.partial(both_step_kernel, "near", int(step), n),
            }[kind]
            held_now = got[f"{part}_{int(step) - 1}"]
            sent[f"{part}_{step}"] = call(kernel, [packet], [sums[part], held_now], 1)


def solution(mesh):
    n, count_x = mesh.shape["gz"], mesh.shape["gx"]
    in_specs = (P(("gx", "gy"), "gz"), P(), P(("gx", "gz"), "gy"))
    out_specs = P(("gx", "gz"), "gy")
    if n != 4 or mesh.shape["gy"] != n or count_x < 2:
        return jax.shard_map(plain, mesh=mesh, in_specs=in_specs, out_specs=out_specs, check_vma=False)

    def body(panels, sizes, front):
        return shards(n, count_x, panels, sizes, front)

    return jax.shard_map(body, mesh=mesh, in_specs=in_specs, out_specs=out_specs, check_vma=False)
```

```python
import functools

import jax
import jax.numpy as jnp
from jax import lax
from jax.experimental import pallas as pl
from jax.experimental.pallas import tpu as pltpu
from jax.sharding import PartitionSpec as P


WIDTH = 1024
GROUP = 64
CODES = 8
STEPS = 256.0
TOP = 32767.0


def plain(panels, sizes, front):
    piece_rows = panels.shape[0]
    panel_count = panels.shape[1] // WIDTH
    first = lax.axis_index("gz") * panel_count
    limits = lax.dynamic_slice_in_dim(sizes, first, panel_count, 0)
    column = jnp.arange(WIDTH, dtype=jnp.int32)
    live = (column[None, :] < limits[:, None]).reshape(panel_count * WIDTH).astype(jnp.bfloat16)
    gathered = lax.all_gather(panels, ("gx", "gy"), axis=0, tiled=True)
    count_x = lax.axis_size("gx")
    count_y = lax.axis_size("gy")
    block_rows = piece_rows * count_y
    row_part = lax.dynamic_slice_in_dim(gathered, lax.axis_index("gx") * block_rows, block_rows, 0)
    grouped = gathered.reshape(count_x, count_y, piece_rows, panels.shape[1])
    column_part = lax.dynamic_index_in_dim(grouped, lax.axis_index("gy"), 1, keepdims=False)
    column_part = column_part.reshape(count_x * piece_rows, panels.shape[1])
    masked = row_part * live[None, :]
    summed = lax.psum_scatter(
        -lax.dot_general(
            masked, column_part, (((1,), (1,)), ((), ())), preferred_element_type=jnp.float32
        ),
        "gz",
        scatter_dimension=0,
        tiled=True,
    )
    return front + summed


def place(rnd, n):
    g = lax.axis_index("gy")
    z = lax.axis_index("gz")
    own_half = g // (n // 2)
    half = own_half if rnd == 0 else 1 - own_half
    w = jnp.where(half == 1, z, n - 1 - z)
    far = jnp.where(half == 1, n - 1, 0)
    return g, w, far


def product(rows, cols):
    return lax.dot_general(rows, cols, (((1,), (1,)), ((), ())), preferred_element_type=jnp.float32)


def decode(packet_ref, group, codes):
    scale = jnp.exp2(codes[group : group + 1, :] * (1.0 / STEPS)) * (1.0 / TOP)
    values = packet_ref[group * GROUP : (group + 1) * GROUP, :].astype(jnp.int32).astype(jnp.float32)
    return values * scale


def read_codes(packet_ref):
    height = packet_ref.shape[0] - CODES
    return packet_ref[height:, :].astype(jnp.int32).astype(jnp.float32)


def encode(out_ref, read):
    height, width = out_ref.shape[0] - CODES, out_ref.shape[1]
    line = lax.broadcasted_iota(jnp.int32, (CODES, width), 0)
    codes = jnp.zeros((CODES, width), jnp.float32)
    for group in range(height // GROUP):
        part = read(group)
        most = jnp.max(jnp.abs(part), axis=0, keepdims=True)
        code = jnp.ceil(jnp.log2(jnp.maximum(most, 1e-30)) * STEPS) + 1.0
        scaled = jnp.round(part * (jnp.exp2(code * (-1.0 / STEPS)) * TOP))
        scaled = jnp.clip(scaled, -TOP, TOP)
        out_ref[group * GROUP : (group + 1) * GROUP, :] = scaled.astype(jnp.int32).astype(jnp.int16)
        codes = jnp.where(line == group, code, codes)
    out_ref[height:, :] = codes.astype(jnp.int32).astype(jnp.int16)


def rows_of(group):
    return slice(group * GROUP, (group + 1) * GROUP)


def rows_of(group):
    return slice(group * GROUP, (group + 1) * GROUP)


def headed(to, n):
    g = lax.axis_index("gy")
    return jnp.where(g // (n // 2) == to // (n // 2), 0, 1)


def at_ends(n):
    g = lax.axis_index("gy")
    return (g == 0) | (g == n - 1)


def own_kernel(n, live, panels, beside, cols, sums, locals_, packet):
    _, w, _ = place(0, n)
    ends = at_ends(n)
    for index, pick in ((0, ends), (1, jnp.logical_not(ends))):
        locals_[index] = jnp.where(pick, panels[...], beside[...]) * live[...]
        sums[index] = product(locals_[index], cols[...])
    at = jnp.where(w == 0, 0, 1)
    encode(packet, lambda group: sums[at, rows_of(group), :])


def own_step_kernel(step, n, sums, held, packet):
    _, w, _ = place(0, n)

    @pl.when((w <= step) & (w >= step - 1))
    def _():
        codes = read_codes(held)
        at = jnp.where(w == step, 0, 1)
        encode(packet, lambda group: sums[at, rows_of(group), :] + decode(held, group, codes))


def far_kernel(n, live, first, second, cols, sums, kept, packet):
    kept[...] = jnp.where(at_ends(n), second[...], first[...]) * live[...]
    sums[...] = product(kept[...], cols[...])
    encode(packet, lambda group: sums[rows_of(group), :])


def near_kernel(kept, cols, sums, packet):
    sums[...] = product(kept[...], cols[...])
    encode(packet, lambda group: sums[rows_of(group), :])


def other_step_kernel(step, n, sums, held, packet):
    _, w, _ = place(1, n)

    @pl.when(w == step)
    def _():
        codes = read_codes(held)
        encode(packet, lambda group: sums[rows_of(group), :] + decode(held, group, codes))


def both_far_kernel(n, locals_, kept, cols, sums, packet):
    z = lax.axis_index("gz")
    sums[0] = product(locals_[0], cols[...])
    sums[1] = product(kept[...], cols[...])

    @pl.when((z == 0) | (z == n - 1))
    def _():
        at = jnp.where(z == 0, headed(n - 1, n), headed(0, n))
        encode(packet, lambda group: sums[at, rows_of(group), :])


def both_near_kernel(n, makes, live, locals_, *rest):
    if makes:
        first, second, *cols, sums, packet, across, kept = rest
        kept[...] = jnp.where(at_ends(n), first[...], second[...]) * live[...]
    else:
        kept, *cols, sums, packet, across = rest
    z = lax.axis_index("gz")
    start = 0
    for part in cols:
        at_columns = slice(start, start + part.shape[0])
        sums[0, :, at_columns] = product(locals_[1], part[...])
        sums[1, :, at_columns] = product(kept[...], part[...])
        start += part.shape[0]

    @pl.when((z == 0) | (z == n - 1))
    def _():
        low, high = headed(1, n), headed(n - 2, n)
        on, off = jnp.where(z == 0, high, low), jnp.where(z == 0, low, high)
        encode(packet, lambda group: sums[on, rows_of(group), :])
        encode(across, lambda group: sums[off, rows_of(group), :])


def both_step_kernel(kind, step, n, sums, held, packet):
    z = lax.axis_index("gz")
    top = n - 2 if kind == "near" else n - 1

    @pl.when((z == step) | (z == n - 1 - step))
    def _():
        codes = read_codes(held)
        at = jnp.where(z == step, headed(top, n), headed(n - 1 - top, n))
        encode(packet, lambda group: sums[at, rows_of(group), :] + decode(held, group, codes))


VMEM = pl.BlockSpec(memory_space=pltpu.VMEM)


def call(kernel, outs, operands, flops):
    size = sum(v.size * v.dtype.itemsize for v in (*operands, *outs))
    return pl.pallas_call(
        kernel,
        out_shape=outs if len(outs) > 1 else outs[0],
        in_specs=[VMEM] * len(operands),
        out_specs=[VMEM] * len(outs) if len(outs) > 1 else VMEM,
        compiler_params=pltpu.CompilerParams(vmem_limit_bytes=min(size + (4 << 20), 60 << 20)),
        cost_estimate=pl.CostEstimate(flops=flops, bytes_accessed=size, transcendentals=0),
    )(*operands)


def crossed_blocks(count_x, rows):
    cut = rows
    return [(d, at, min(cut, rows - at)) for d in range(1, count_x) for at in range(0, rows, cut)]


def base_kernel(n, count_x, blocks, front, *rest):
    sums, out_ref = rest[:-1], rest[-1]
    x = lax.axis_index("gx")
    z = lax.axis_index("gz")
    rows = front.shape[0]
    _, w, _ = place(0, n)

    def columns(d, at=0, size=rows):
        return pl.ds(pl.multiple_of(lax.rem(x + d, count_x) * rows + at, 128), size)

    @pl.when(w >= n // 2)
    def _():
        at = jnp.where(w == n - 1, 0, 1)
        out_ref[:, columns(0)] = front[:, columns(0)] - sums[0][at]

    for at_w, index in ((0, 1), (1, 2)):

        @pl.when(w == at_w)
        def _(index=index):
            out_ref[:, columns(0)] = front[:, columns(0)] - sums[index][...]

    edge = (z == 0) | (z == n - 1)
    mine = jnp.where(w >= n // 2, 0, 1)

    @pl.when(edge)
    def _():
        for index, place_of in enumerate(blocks):
            out_ref[:, columns(*place_of)] = front[:, columns(*place_of)] - sums[3 + index][mine]

    @pl.when(jnp.logical_not(edge))
    def _():
        for d in range(1, count_x):
            out_ref[:, columns(d)] = front[:, columns(d)] - sums[2 + len(blocks) + d][mine]


def final_kernel(n, count_x, blocks, base, *rest):
    packets, out_ref = rest[:-1], rest[-1]
    x = lax.axis_index("gx")
    z = lax.axis_index("gz")
    rows = base.shape[0]
    _, w, _ = place(0, n)

    def finish(place_of, picks):
        d, at, size = place_of
        columns = pl.ds(pl.multiple_of(lax.rem(x + d, count_x) * rows + at, 128), size)
        refs = [packets[k] for k in picks]
        codes = [read_codes(ref) for ref in refs]
        for group in range(rows // GROUP):
            value = base[rows_of(group), columns]
            for ref, code in zip(refs, codes):
                value = value - decode(ref, group, code)
            out_ref[rows_of(group), columns] = value

    for at, picks in ((n - 1, (1,)), (n - 2, (0, 1)), (0, (2,)), (1, (3, 4))):

        @pl.when(w == at)
        def _(picks=picks):
            finish((0, 0, rows), picks)

    edge = (z == 0) | (z == n - 1)

    @pl.when(edge)
    def _():
        for index, place_of in enumerate(blocks):
            finish(place_of, (5 + index,))

    @pl.when(jnp.logical_not(edge))
    def _():
        first = 5 + len(blocks)
        for d in range(1, count_x):
            finish((d, 0, rows), (first + 2 * d - 2, first + 2 * d - 1))


def plan(count_x, blocks):
    crossed = range(1, count_x)
    ends = range(1, blocks + 1)

    def go(label, step):
        return [f"{label}_k{step}", f">{label}_{step}"]

    names = [">beside", ">far0"] + [f">cross{c}" for c in ends] + [">near0"]
    names += go("own", 0) + go("own", 1) + [">far1"] + go("far", 0)
    for c in ends:
        if c == blocks:
            names += go("own", 2) + [">near1"]
        names += go(f"xf{c}", 0)
    names += go("far", 1)
    for d in crossed:
        names += go(f"xn{d}", 0)
    names += go("near", 0)
    for d in crossed:
        names += [f">xn{d}_x"]
    for c in ends:
        names += go(f"xf{c}", 1)
    names += go("far", 2)
    for d in crossed:
        names += go(f"xn{d}", 1)
    for c in ends:
        names += go(f"xf{c}", 2)
    return names + go("near", 1) + ["base", "final"]


def shards(n, count_x, panels, sizes, front):
    rows, width = panels.shape
    square = 2 * rows * rows * width
    one_sum = jax.ShapeDtypeStruct((rows, rows), jnp.float32)
    piece_like = jax.ShapeDtypeStruct((rows, width), jnp.bfloat16)

    def pair_of_sums(size):
        return jax.ShapeDtypeStruct((2, rows, size), jnp.float32)

    def packet(size):
        return jax.ShapeDtypeStruct((rows + CODES, size), jnp.int16)

    block = jax.ShapeDtypeStruct(front.shape, jnp.float32)

    def way(rnd, hops):
        pairs = []
        for g in range(n):
            half = g // (n // 2) if rnd == 0 else 1 - g // (n // 2)
            for a, b in hops:
                source, target = (a, b) if half == 1 else (n - 1 - a, n - 1 - b)
                pairs.append((g * n + source, g * n + target))
        return pairs

    def both(hop):
        return way(0, [hop]) + way(1, [hop])

    count = width // WIDTH
    here = jnp.arange(sizes.size, dtype=jnp.int32)[:, None] == lax.axis_index("gz") * count + jnp.arange(count)[None, :]
    limits = jnp.sum(jnp.where(here, sizes[:, None], 0), axis=0)
    live = (jnp.arange(WIDTH)[None, :] < limits[:, None]).reshape(1, width).astype(jnp.bfloat16)

    hops = {
        "own_0": way(0, [(0, 1), (n - 1, n - 2)]),
        "own_1": way(0, [(0, 1), (1, 2)]),
        "own_2": way(0, [(1, 2), (2, 3)]),
        "far_0": way(1, [(0, 1)]),
        "far_1": way(1, [(1, 2)]),
        "far_2": way(1, [(2, 3)]),
        "near_0": way(1, [(0, 1), (n - 1, n - 2)]),
        "near_1": way(1, [(1, 2)]),
        "xf_0": both((0, 1)),
        "xf_1": both((1, 2)),
        "xf_2": both((2, 3)),
        "xn_0": both((0, 1)),
        "xn_1": both((1, 2)),
        "xn_x": both((n - 1, n - 2)),
    }
    y_moves = {
        "beside": (None, [(g, g ^ 1) for g in range(n)]),
        "far0": (None, [(0, 2), (3, 1)]),
        "near0": ("beside", [(0, 3), (3, 0)]),
        "far1": ("far0", [(2, 3), (1, 0)]),
        "near1": ("near0", [(3, 2), (0, 1)]),
    }
    blocks = crossed_blocks(count_x, rows)
    held = {}
    sums = {}
    sent = {}
    got = {}
    for name in plan(count_x, len(blocks)):
        label = name.lstrip(">")
        part, _, step = label.partition("_")
        step = step.lstrip("k")
        kind, c = part.rstrip("0123456789"), int("0" + part.lstrip("abcdefghijklmnopqrstuvwxyz"))
        if label in y_moves:
            source, pairs = y_moves[label]
            held[label] = lax.ppermute(panels if source is None else held[source], "gy", pairs)
        elif kind == "cross":
            d, at, size = blocks[c - 1]
            piece = panels if size == rows else lax.slice_in_dim(panels, at, at + size, axis=0)
            held[label] = lax.ppermute(piece, "gx", [((i + d) % count_x, i) for i in range(count_x)])
        elif name[0] == ">":
            got[label] = lax.ppermute(sent[label], ("gy", "gz"), hops[f"{kind}_{step}"])
        elif label == "base":
            each = [sums[k] for k in ("own", "far", "near")]
            each += [sums[f"xf{c + 1}"] for c in range(len(blocks))] + [sums[f"xn{d}"] for d in range(1, count_x)]
            base = call(functools.partial(base_kernel, n, count_x, blocks), [block], [front, *each], 1)
        elif label == "final":
            each = [got[k] for k in ("own_0", "own_2", "far_2", "near_0", "near_1")]
            each += [got[f"xf{c + 1}_2"] for c in range(len(blocks))]
            each += [got[f"xn{d}_{k}"] for d in range(1, count_x) for k in ("1", "x")]
            return call(functools.partial(final_kernel, n, count_x, blocks), [block], [base, *each], 1)
        elif step != "0":
            kernel = {
                "own": functools.partial(own_step_kernel, int(step), n),
                "far": functools.partial(other_step_kernel, int(step), n),
                "near": functools.partial(other_step_kernel, int(step), n),
                "xf": functools.partial(both_step_kernel, "far", int(step), n),
                "xn": functools.partial(both_step_kernel, "near", int(step), n),
            }[kind]
            before = got[f"{part}_{int(step) - 1}"]
            sent[f"{part}_{step}"] = call(kernel, [packet(before.shape[1])], [sums[part], before], 1)
        elif kind == "own":
            sums[part], held["locals"], sent["own_0"] = call(
                functools.partial(own_kernel, n),
                [pair_of_sums(rows), jax.ShapeDtypeStruct((2, rows, width), jnp.bfloat16), packet(rows)],
                [live, panels, held["beside"], panels],
                2 * square,
            )
        elif kind == "far":
            sums[part], held["kept_far"], sent["far_0"] = call(
                functools.partial(far_kernel, n),
                [one_sum, piece_like, packet(rows)],
                [live, held["far0"], held["far1"], panels],
                square,
            )
        elif kind == "near":
            sums[part], sent["near_0"] = call(near_kernel, [one_sum, packet(rows)], [held["kept_near"], panels], square)
        elif kind == "xf":
            size = blocks[c - 1][2]
            sums[part], sent[f"{part}_0"] = call(
                functools.partial(both_far_kernel, n),
                [pair_of_sums(size), packet(size)],
                [held["locals"], held["kept_far"], held[f"cross{c}"]],
                4 * rows * size * width,
            )
        else:
            makes = "kept_near" not in held
            pieces = (held["near0"], held["near1"]) if makes else (held["kept_near"],)
            cols = [held[f"cross{i + 1}"] for i, block_of in enumerate(blocks) if block_of[0] == c]
            done = call(
                functools.partial(both_near_kernel, n, makes),
                [pair_of_sums(rows), packet(rows), packet(rows)] + [piece_like] * makes,
                [live, held["locals"], *pieces, *cols],
                2 * square,
            )
            sums[part], sent[f"{part}_0"], sent[f"{part}_x"] = done[:3]
            if makes:
                held["kept_near"] = done[3]


def solution(mesh):
    n, count_x = mesh.shape["gz"], mesh.shape["gx"]
    in_specs = (P(("gx", "gy"), "gz"), P(), P(("gx", "gz"), "gy"))
    out_specs = P(("gx", "gz"), "gy")
    if n != 4 or mesh.shape["gy"] != n or count_x < 2:
        return jax.shard_map(plain, mesh=mesh, in_specs=in_specs, out_specs=out_specs, check_vma=False)

    def body(panels, sizes, front):
        return shards(n, count_x, panels, sizes, front)

    return jax.shard_map(body, mesh=mesh, in_specs=in_specs, out_specs=out_specs, check_vma=False)
```

```python
import functools

import jax
import jax.numpy as jnp
from jax import lax
from jax.experimental import pallas as pl
from jax.experimental.pallas import tpu as pltpu
from jax.sharding import PartitionSpec as P


WIDTH = 1024
GROUP = 64
CODES = 8
STEPS = 256.0
TOP = 32767.0


def plain(panels, sizes, front):
    piece_rows = panels.shape[0]
    panel_count = panels.shape[1] // WIDTH
    first = lax.axis_index("gz") * panel_count
    limits = lax.dynamic_slice_in_dim(sizes, first, panel_count, 0)
    column = jnp.arange(WIDTH, dtype=jnp.int32)
    live = (column[None, :] < limits[:, None]).reshape(panel_count * WIDTH).astype(jnp.bfloat16)
    gathered = lax.all_gather(panels, ("gx", "gy"), axis=0, tiled=True)
    count_x = lax.axis_size("gx")
    count_y = lax.axis_size("gy")
    block_rows = piece_rows * count_y
    row_part = lax.dynamic_slice_in_dim(gathered, lax.axis_index("gx") * block_rows, block_rows, 0)
    grouped = gathered.reshape(count_x, count_y, piece_rows, panels.shape[1])
    column_part = lax.dynamic_index_in_dim(grouped, lax.axis_index("gy"), 1, keepdims=False)
    column_part = column_part.reshape(count_x * piece_rows, panels.shape[1])
    masked = row_part * live[None, :]
    summed = lax.psum_scatter(
        -lax.dot_general(
            masked, column_part, (((1,), (1,)), ((), ())), preferred_element_type=jnp.float32
        ),
        "gz",
        scatter_dimension=0,
        tiled=True,
    )
    return front + summed


def place(rnd, n):
    g = lax.axis_index("gy")
    z = lax.axis_index("gz")
    own_half = g // (n // 2)
    half = own_half if rnd == 0 else 1 - own_half
    w = jnp.where(half == 1, z, n - 1 - z)
    far = jnp.where(half == 1, n - 1, 0)
    return g, w, far


def product(rows, cols):
    return lax.dot_general(rows, cols[...], (((1,), (1,)), ((), ())), preferred_element_type=jnp.float32)


def decode(packet_ref, group, codes):
    scale = jnp.exp2(codes[group : group + 1, :] * (1.0 / STEPS)) * (1.0 / TOP)
    values = packet_ref[group * GROUP : (group + 1) * GROUP, :].astype(jnp.int32).astype(jnp.float32)
    return values * scale


def read_codes(packet_ref):
    height = packet_ref.shape[0] - CODES
    return packet_ref[height:, :].astype(jnp.int32).astype(jnp.float32)


def encode(out_ref, read):
    height, width = out_ref.shape[0] - CODES, out_ref.shape[1]
    line = lax.broadcasted_iota(jnp.int32, (CODES, width), 0)
    codes = jnp.zeros((CODES, width), jnp.float32)
    for group in range(height // GROUP):
        part = read(group)
        most = jnp.max(jnp.abs(part), axis=0, keepdims=True)
        code = jnp.ceil(jnp.log2(jnp.maximum(most, 1e-30)) * STEPS) + 1.0
        scaled = jnp.round(part * (jnp.exp2(code * (-1.0 / STEPS)) * TOP))
        scaled = jnp.clip(scaled, -TOP, TOP)
        out_ref[group * GROUP : (group + 1) * GROUP, :] = scaled.astype(jnp.int32).astype(jnp.int16)
        codes = jnp.where(line == group, code, codes)
    out_ref[height:, :] = codes.astype(jnp.int32).astype(jnp.int16)


def rows_of(group):
    return slice(group * GROUP, (group + 1) * GROUP)


def rows_of(group):
    return slice(group * GROUP, (group + 1) * GROUP)


def headed(to, n):
    g = lax.axis_index("gy")
    return jnp.where(g // (n // 2) == to // (n // 2), 0, 1)


def at_ends(n):
    g = lax.axis_index("gy")
    return (g == 0) | (g == n - 1)


def own_kernel(n, live, panels, beside, cols, sums, locals_, packet, other):
    _, w, _ = place(0, n)
    ends = at_ends(n)
    for index, pick in ((0, ends), (1, jnp.logical_not(ends))):
        locals_[index] = jnp.where(pick, panels[...], beside[...]) * live[...]
        sums[index] = product(locals_[index], cols)
    at = jnp.where((w == 0) | (w == 2), 0, 1)
    encode(packet, lambda group: sums[at, rows_of(group), :])

    @pl.when(w < 2)
    def _():
        encode(other, lambda group: sums[1 - at, rows_of(group), :])


def far_kernel(n, live, first, second, cols, sums, kept, packet):
    kept[...] = jnp.where(at_ends(n), second[...], first[...]) * live[...]
    sums[...] = product(kept[...], cols)
    encode(packet, lambda group: sums[rows_of(group), :])


def near_kernel(kept, cols, sums, packet):
    sums[...] = product(kept[...], cols)
    encode(packet, lambda group: sums[rows_of(group), :])


def near_step_kernel(n, sums, held, packet):
    _, w, _ = place(1, n)

    @pl.when(w == 1)
    def _():
        codes = read_codes(held)
        encode(packet, lambda group: sums[rows_of(group), :] + decode(held, group, codes))


def early(kind, n):
    z = lax.axis_index("gz")
    top = n - 1 if kind == "xf" else n - 2
    return jnp.where(z < n // 2, headed(top, n), headed(n - 1 - top, n))


def at_edge(n):
    z = lax.axis_index("gz")
    return (z == 0) | (z == n - 1)


def crossed_kernel(kind, is_early, makes, n, *rest):
    if makes:
        live, locals_, first, second, cols, sums, packet, kept = rest
        kept[...] = jnp.where(at_ends(n), first[...], second[...]) * live[...]
    else:
        locals_, kept, cols, sums, *packet = rest
        packet = packet[0] if packet else None
    at = early(kind, n) if is_early else 1 - early(kind, n)

    @pl.when(at == 0)
    def _():
        sums[...] = product(locals_[0 if kind == "xf" else 1], cols)

    @pl.when(at == 1)
    def _():
        sums[...] = product(kept[...], cols)

    if packet is not None:

        @pl.when(at_edge(n))
        def _():
            encode(packet, lambda group: sums[rows_of(group), :])


def crossed_step_kernel(n, sums, held, packet):
    @pl.when(jnp.logical_not(at_edge(n)))
    def _():
        codes = read_codes(held)
        encode(packet, lambda group: sums[rows_of(group), :] + decode(held, group, codes))


def last_kernel(n, far_late, held, near_late, packet):
    @pl.when(at_edge(n))
    def _():
        encode(packet, lambda group: near_late[rows_of(group), :])

    @pl.when(jnp.logical_not(at_edge(n)))
    def _():
        codes = read_codes(held)
        encode(packet, lambda group: far_late[rows_of(group), :] + decode(held, group, codes))


VMEM = pl.BlockSpec(memory_space=pltpu.VMEM)


def call(kernel, outs, operands, flops):
    size = sum(v.size * v.dtype.itemsize for v in (*operands, *outs))
    return pl.pallas_call(
        kernel,
        out_shape=outs if len(outs) > 1 else outs[0],
        in_specs=[VMEM] * len(operands),
        out_specs=[VMEM] * len(outs) if len(outs) > 1 else VMEM,
        compiler_params=pltpu.CompilerParams(vmem_limit_bytes=min(size + (4 << 20), 60 << 20)),
        cost_estimate=pl.CostEstimate(flops=flops, bytes_accessed=size, transcendentals=0),
    )(*operands)


def subtract(out_ref, value_ref, columns, refs):
    codes = [read_codes(ref) for ref in refs]
    for group in range(out_ref.shape[0] // GROUP):
        value = value_ref[rows_of(group), columns]
        for ref, code in zip(refs, codes):
            value = value - decode(ref, group, code)
        out_ref[rows_of(group), columns] = value


def own_columns(count_x, rows, d):
    return pl.ds(pl.multiple_of(lax.rem(lax.axis_index("gx") + d, count_x) * rows, 128), rows)


def base_kernel(n, count_x, front, *rest):
    packets, sums, out_ref = rest[:6], rest[6:-1], rest[-1]
    z = lax.axis_index("gz")
    rows = front.shape[0]
    _, w, _ = place(0, n)
    columns = functools.partial(own_columns, count_x, rows)

    @pl.when(w >= n // 2)
    def _():
        at = jnp.where(w == n - 1, 0, 1)
        out_ref[:, columns(0)] = front[:, columns(0)] - sums[0][at]
        subtract(out_ref, out_ref, columns(0), packets[:3])

    @pl.when(w == 0)
    def _():
        out_ref[:, columns(0)] = front[:, columns(0)] - sums[1][...]
        subtract(out_ref, out_ref, columns(0), packets[3:])

    @pl.when(w == 1)
    def _():
        out_ref[:, columns(0)] = front[:, columns(0)] - sums[2][...]

    edge = (z == 0) | (z == n - 1)
    for d in range(1, count_x):
        for side, index in ((edge, 1 + 2 * d), (jnp.logical_not(edge), 2 + 2 * d)):

            @pl.when(side)
            def _(d=d, index=index):
                out_ref[:, columns(d)] = front[:, columns(d)] - sums[index][...]


def final_kernel(n, count_x, base, *rest):
    packets, out_ref = rest[:-1], rest[-1]
    z = lax.axis_index("gz")
    rows = base.shape[0]
    _, w, _ = place(0, n)
    columns = functools.partial(own_columns, count_x, rows)

    @pl.when(w == 1)
    def _():
        subtract(out_ref, base, columns(0), packets[:2])

    @pl.when(w != 1)
    def _():
        out_ref[:, columns(0)] = base[:, columns(0)]

    edge = (z == 0) | (z == n - 1)
    for d in range(1, count_x):
        for side, refs in ((edge, packets[2 * d : 2 * d + 1]), (jnp.logical_not(edge), packets[2 * d : 2 * d + 2])):

            @pl.when(side)
            def _(d=d, refs=refs):
                subtract(out_ref, base, columns(d), refs)


def plan(count_x):
    crossed = range(1, count_x)
    names = [">beside", ">far0"] + [f">cross{d}" for d in crossed] + [">near0"]
    names += ["own_k", ">own_a", ">own_b", ">own_c", ">far1", "far_k", ">far_a", ">far_b", ">far_c", ">near1"]
    for d in crossed:
        names += [f"xf{d}_k", f">xf{d}_0"]
    for d in crossed:
        names += [f"xn{d}_k", f">xn{d}_0"]
    names += ["near_k", ">near_0"]
    for d in crossed:
        names += [f"xf{d}_j1", f">xf{d}_1", f"xn{d}_m", f"xf{d}_m"]
    for d in crossed:
        names += [f"xn{d}_j1", f">xn{d}_1"]
    for d in crossed:
        names += [f"last{d}_k", f">last{d}_0"]
    return names + ["base", "near_j1", ">near_1", "final"]


def shards(n, count_x, panels, sizes, front):
    rows, width = panels.shape
    square = 2 * rows * rows * width
    one_sum = jax.ShapeDtypeStruct((rows, rows), jnp.float32)
    piece_like = jax.ShapeDtypeStruct((rows, width), jnp.bfloat16)

    block = jax.ShapeDtypeStruct(front.shape, jnp.float32)

    def way(rnd, hops):
        pairs = []
        for g in range(n):
            half = g // (n // 2) if rnd == 0 else 1 - g // (n // 2)
            for a, b in hops:
                source, target = (a, b) if half == 1 else (n - 1 - a, n - 1 - b)
                pairs.append((g * n + source, g * n + target))
        return pairs

    def both(hop):
        return way(0, [hop]) + way(1, [hop])

    count = width // WIDTH
    here = jnp.arange(sizes.size, dtype=jnp.int32)[:, None] == lax.axis_index("gz") * count + jnp.arange(count)[None, :]
    limits = jnp.sum(jnp.where(here, sizes[:, None], 0), axis=0)
    live = (jnp.arange(WIDTH)[None, :] < limits[:, None]).reshape(1, width).astype(jnp.bfloat16)

    hops = {
        "own_a": way(0, [(0, 3), (1, 2)]),
        "own_b": way(0, [(0, 2), (1, 3)]),
        "own_c": way(0, [(2, 3), (3, 2)]),
        "far_a": way(1, [(0, 3)]),
        "far_b": way(1, [(1, 3)]),
        "far_c": way(1, [(2, 3)]),
        "near_0": way(1, [(0, 1), (3, 2)]),
        "near_1": way(1, [(1, 2)]),
        "xf_0": both((0, 1)),
        "xf_1": both((1, 2)),
        "last_0": both((2, 3)) + both((3, 2)),
        "xn_0": both((0, 1)),
        "xn_1": both((1, 2)),
    }
    y_moves = {
        "beside": (None, [(g, g ^ 1) for g in range(n)]),
        "far0": (None, [(0, 2), (3, 1)]),
        "near0": ("beside", [(0, 3), (3, 0)]),
        "far1": ("far0", [(2, 3), (1, 0)]),
        "near1": ("near0", [(3, 2), (0, 1)]),
    }
    held = {}
    sums = {}
    sent = {}
    got = {}
    pair_of_sums = jax.ShapeDtypeStruct((2, rows, rows), jnp.float32)
    packet = jax.ShapeDtypeStruct((rows + CODES, rows), jnp.int16)
    for name in plan(count_x):
        label = name.lstrip(">")
        part, _, step = label.partition("_")
        kind, d = part.rstrip("0123456789"), int("0" + part.lstrip("abcdefghijklmnopqrstuvwxyz"))
        if label in y_moves:
            source, pairs = y_moves[label]
            held[label] = lax.ppermute(panels if source is None else held[source], "gy", pairs)
        elif kind == "cross":
            held[label] = lax.ppermute(panels, "gx", [((i + d) % count_x, i) for i in range(count_x)])
        elif name[0] == ">":
            got[label] = lax.ppermute(sent[label], ("gy", "gz"), hops[f"{kind}_{step}"])
        elif label == "base":
            each = [got[f"{k}_{i}"] for k in ("own", "far") for i in "abc"]
            each += [sums[k] for k in ("own", "far", "near")]
            each += [sums[f"{k}{d}", "late"] for d in range(1, count_x) for k in ("xf", "xn")]
            base = call(functools.partial(base_kernel, n, count_x), [block], [front, *each], 1)
        elif label == "final":
            each = [got["near_0"], got["near_1"]]
            for d in range(1, count_x):
                each += [got[f"last{d}_0"], got[f"xn{d}_1"]]
            return call(functools.partial(final_kernel, n, count_x), [block], [base, *each], 1)
        elif step[0] == "j":
            at = int(step[1])
            kernel = near_step_kernel if kind == "near" else crossed_step_kernel
            which = part if kind == "near" else (part, "early" if at == 1 else "late")
            before = got[f"{part}_{at - 1}"]
            sent[f"{part}_{at}"] = call(functools.partial(kernel, n), [packet], [sums[which], before], 1)
        elif kind == "last":
            sent[f"{part}_0"] = call(
                functools.partial(last_kernel, n),
                [packet],
                [sums[f"xf{d}", "late"], got[f"xf{d}_1"], sums[f"xn{d}", "late"]],
                1,
            )
        elif kind == "own":
            sums[part], held["locals"], sent["own_a"], sent["own_b"] = call(
                functools.partial(own_kernel, n),
                [pair_of_sums, jax.ShapeDtypeStruct((2, rows, width), jnp.bfloat16), packet, packet],
                [live, panels, held["beside"], panels],
                2 * square,
            )
            sent["own_c"] = sent["own_a"]
        elif kind == "far":
            sums[part], held["kept_far"], sent["far_a"] = call(
                functools.partial(far_kernel, n),
                [one_sum, piece_like, packet],
                [live, held["far0"], held["far1"], panels],
                square,
            )
            sent["far_b"] = sent["far_c"] = sent["far_a"]
        elif kind == "near":
            sums[part], sent["near_0"] = call(near_kernel, [one_sum, packet], [held["kept_near"], panels], square)
        else:
            is_early = step == "k"
            kept = "kept_far" if kind == "xf" else "kept_near"
            makes = kept not in held
            pieces = [held["near0"], held["near1"]] if makes else [held[kept]]
            packs = is_early
            done = call(
                functools.partial(crossed_kernel, kind, is_early, makes, n),
                [one_sum] + [packet] * packs + [piece_like] * makes,
                [live] * makes + [held["locals"], *pieces, held[f"cross{d}"]],
                square,
            )
            done = done if isinstance(done, (tuple, list)) else [done]
            sums[part, "early" if is_early else "late"] = done[0]
            if packs:
                sent[f"{part}_0"] = done[1]
            if makes:
                held[kept] = done[2]


def solution(mesh):
    n, count_x = mesh.shape["gz"], mesh.shape["gx"]
    in_specs = (P(("gx", "gy"), "gz"), P(), P(("gx", "gz"), "gy"))
    out_specs = P(("gx", "gz"), "gy")
    if n != 4 or mesh.shape["gy"] != n or count_x < 2:
        return jax.shard_map(plain, mesh=mesh, in_specs=in_specs, out_specs=out_specs, check_vma=False)

    def body(panels, sizes, front):
        return shards(n, count_x, panels, sizes, front)

    return jax.shard_map(body, mesh=mesh, in_specs=in_specs, out_specs=out_specs, check_vma=False)
```

```python
import functools

import jax
import jax.numpy as jnp
from jax import lax
from jax.experimental import pallas as pl
from jax.experimental.pallas import tpu as pltpu
from jax.sharding import PartitionSpec as P


WIDTH = 1024
GROUP = 64
CODES = 8
STEPS = 256.0
TOP = 32767.0


def plain(panels, sizes, front):
    piece_rows = panels.shape[0]
    panel_count = panels.shape[1] // WIDTH
    first = lax.axis_index("gz") * panel_count
    limits = lax.dynamic_slice_in_dim(sizes, first, panel_count, 0)
    column = jnp.arange(WIDTH, dtype=jnp.int32)
    live = (column[None, :] < limits[:, None]).reshape(panel_count * WIDTH).astype(jnp.bfloat16)
    gathered = lax.all_gather(panels, ("gx", "gy"), axis=0, tiled=True)
    count_x = lax.axis_size("gx")
    count_y = lax.axis_size("gy")
    block_rows = piece_rows * count_y
    row_part = lax.dynamic_slice_in_dim(gathered, lax.axis_index("gx") * block_rows, block_rows, 0)
    grouped = gathered.reshape(count_x, count_y, piece_rows, panels.shape[1])
    column_part = lax.dynamic_index_in_dim(grouped, lax.axis_index("gy"), 1, keepdims=False)
    column_part = column_part.reshape(count_x * piece_rows, panels.shape[1])
    masked = row_part * live[None, :]
    summed = lax.psum_scatter(
        -lax.dot_general(
            masked, column_part, (((1,), (1,)), ((), ())), preferred_element_type=jnp.float32
        ),
        "gz",
        scatter_dimension=0,
        tiled=True,
    )
    return front + summed


def place(rnd, n):
    g = lax.axis_index("gy")
    z = lax.axis_index("gz")
    own_half = g // (n // 2)
    half = own_half if rnd == 0 else 1 - own_half
    w = jnp.where(half == 1, z, n - 1 - z)
    far = jnp.where(half == 1, n - 1, 0)
    return g, w, far


def product(rows, cols):
    return lax.dot_general(rows, cols[...], (((1,), (1,)), ((), ())), preferred_element_type=jnp.float32)


def decode(packet_ref, group, codes):
    scale = jnp.exp2(codes[group : group + 1, :] * (1.0 / STEPS)) * (1.0 / TOP)
    values = packet_ref[group * GROUP : (group + 1) * GROUP, :].astype(jnp.int32).astype(jnp.float32)
    return values * scale


def read_codes(packet_ref):
    height = packet_ref.shape[0] - CODES
    return packet_ref[height:, :].astype(jnp.int32).astype(jnp.float32)


def encode(out_ref, read):
    height, width = out_ref.shape[0] - CODES, out_ref.shape[1]
    line = lax.broadcasted_iota(jnp.int32, (CODES, width), 0)
    codes = jnp.zeros((CODES, width), jnp.float32)
    for group in range(height // GROUP):
        part = read(group)
        most = jnp.max(jnp.abs(part), axis=0, keepdims=True)
        code = jnp.ceil(jnp.log2(jnp.maximum(most, 1e-30)) * STEPS) + 1.0
        scaled = jnp.round(part * (jnp.exp2(code * (-1.0 / STEPS)) * TOP))
        scaled = jnp.clip(scaled, -TOP, TOP)
        out_ref[group * GROUP : (group + 1) * GROUP, :] = scaled.astype(jnp.int32).astype(jnp.int16)
        codes = jnp.where(line == group, code, codes)
    out_ref[height:, :] = codes.astype(jnp.int32).astype(jnp.int16)


def rows_of(group):
    return slice(group * GROUP, (group + 1) * GROUP)


def rows_of(group):
    return slice(group * GROUP, (group + 1) * GROUP)


def headed(to, n):
    g = lax.axis_index("gy")
    return jnp.where(g // (n // 2) == to // (n // 2), 0, 1)


def at_ends(n):
    g = lax.axis_index("gy")
    return (g == 0) | (g == n - 1)


def own_kernel(n, live, panels, beside, cols, sums, locals_, packet, other):
    _, w, _ = place(0, n)
    ends = at_ends(n)
    for index, pick in ((0, ends), (1, jnp.logical_not(ends))):
        locals_[index] = jnp.where(pick, panels[...], beside[...]) * live[...]
        sums[index] = product(locals_[index], cols)
    at = jnp.where((w == 0) | (w == 2), 0, 1)
    encode(packet, lambda group: sums[at, rows_of(group), :])

    @pl.when(w < 2)
    def _():
        encode(other, lambda group: sums[1 - at, rows_of(group), :])


def far_kernel(n, live, first, second, cols, sums, kept, packet):
    kept[...] = jnp.where(at_ends(n), second[...], first[...]) * live[...]
    sums[...] = product(kept[...], cols)
    encode(packet, lambda group: sums[rows_of(group), :])


def near_kernel(kept, cols, sums, packet):
    sums[...] = product(kept[...], cols)
    encode(packet, lambda group: sums[rows_of(group), :])


def near_step_kernel(n, sums, held, packet):
    _, w, _ = place(1, n)

    @pl.when(w == 1)
    def _():
        codes = read_codes(held)
        encode(packet, lambda group: sums[rows_of(group), :] + decode(held, group, codes))


def early(kind, n):
    z = lax.axis_index("gz")
    top = n - 1 if kind == "xf" else n - 2
    return jnp.where(z < n // 2, headed(top, n), headed(n - 1 - top, n))


def at_edge(n):
    z = lax.axis_index("gz")
    return (z == 0) | (z == n - 1)


def crossed_kernel(kind, is_early, makes, n, *rest):
    if makes:
        live, locals_, first, second, cols, sums, packet, kept = rest
        kept[...] = jnp.where(at_ends(n), first[...], second[...]) * live[...]
    else:
        locals_, kept, cols, sums, *packet = rest
        packet = packet[0] if packet else None
    at = early(kind, n) if is_early else 1 - early(kind, n)

    @pl.when(at == 0)
    def _():
        sums[...] = product(locals_[0 if kind == "xf" else 1], cols)

    @pl.when(at == 1)
    def _():
        sums[...] = product(kept[...], cols)

    if packet is not None:

        @pl.when(at_edge(n))
        def _():
            encode(packet, lambda group: sums[rows_of(group), :])


def crossed_step_kernel(n, sums, held, packet):
    @pl.when(jnp.logical_not(at_edge(n)))
    def _():
        codes = read_codes(held)
        encode(packet, lambda group: sums[rows_of(group), :] + decode(held, group, codes))


def last_kernel(n, far_late, held, near_late, packet):
    @pl.when(at_edge(n))
    def _():
        encode(packet, lambda group: near_late[rows_of(group), :])

    @pl.when(jnp.logical_not(at_edge(n)))
    def _():
        codes = read_codes(held)
        encode(packet, lambda group: far_late[rows_of(group), :] + decode(held, group, codes))


VMEM = pl.BlockSpec(memory_space=pltpu.VMEM)


def call(kernel, outs, operands, flops):
    size = sum(v.size * v.dtype.itemsize for v in (*operands, *outs))
    return pl.pallas_call(
        kernel,
        out_shape=outs if len(outs) > 1 else outs[0],
        in_specs=[VMEM] * len(operands),
        out_specs=[VMEM] * len(outs) if len(outs) > 1 else VMEM,
        compiler_params=pltpu.CompilerParams(vmem_limit_bytes=min(size + (4 << 20), 60 << 20)),
        cost_estimate=pl.CostEstimate(flops=flops, bytes_accessed=size, transcendentals=0),
    )(*operands)


def subtract(out_ref, value_ref, columns, refs):
    codes = [read_codes(ref) for ref in refs]
    for group in range(out_ref.shape[0] // GROUP):
        value = value_ref[rows_of(group), columns]
        for ref, code in zip(refs, codes):
            value = value - decode(ref, group, code)
        out_ref[rows_of(group), columns] = value


def own_columns(count_x, rows, d):
    return pl.ds(pl.multiple_of(lax.rem(lax.axis_index("gx") + d, count_x) * rows, 128), rows)


def base_kernel(n, count_x, front, *rest):
    middle = 7 + 2 * (count_x - 1)
    packets, sums, out_ref = rest[:middle], rest[middle:-1], rest[-1]
    rows = front.shape[0]
    _, w, _ = place(0, n)
    columns = functools.partial(own_columns, count_x, rows)

    def settle(d, own, refs):
        out_ref[:, columns(d)] = front[:, columns(d)] - own
        subtract(out_ref, out_ref, columns(d), refs)

    @pl.when(w >= n // 2)
    def _():
        settle(0, sums[0][jnp.where(w == n - 1, 0, 1)], packets[:3])

    @pl.when(w == 0)
    def _():
        settle(0, sums[1][...], packets[3:6])

    @pl.when(w == 1)
    def _():
        settle(0, sums[2][...], packets[6:7])

    edge = at_edge(n)
    for d in range(1, count_x):
        first = 5 + 2 * d

        @pl.when(edge)
        def _(d=d, first=first):
            settle(d, sums[1 + 2 * d][...], packets[first : first + 1])

        @pl.when(jnp.logical_not(edge))
        def _(d=d, first=first):
            settle(d, sums[2 + 2 * d][...], packets[first : first + 2])


def final_kernel(n, count_x, base, packet, out_ref):
    _, w, _ = place(0, n)
    out_ref[...] = base[...]

    @pl.when(w == 1)
    def _():
        subtract(out_ref, base, own_columns(count_x, base.shape[0], 0), [packet])


def plan(count_x):
    crossed = range(1, count_x)
    names = [">beside", ">far0"] + [f">cross{d}" for d in crossed] + [">near0"]
    names += ["own_k", ">own_c", ">own_a", ">own_b", ">far1", "far_k", ">far_a", ">far_b", ">far_c", ">near1"]
    for d in crossed:
        names += [f"xf{d}_k", f">xf{d}_0"]
    for d in crossed:
        names += [f"xn{d}_k", f">xn{d}_0"]
    names += ["near_k", ">near_0"]
    for d in crossed:
        names += [f"xf{d}_j1", f">xf{d}_1", f"xn{d}_m", f"xf{d}_m"]
    for d in crossed:
        names += [f"xn{d}_j1", f">xn{d}_1"]
    for d in crossed:
        names += [f"last{d}_k", f">last{d}_0"]
    return names + ["near_j1", ">near_1", "base", "final"]


def shards(n, count_x, panels, sizes, front):
    rows, width = panels.shape
    square = 2 * rows * rows * width
    one_sum = jax.ShapeDtypeStruct((rows, rows), jnp.float32)
    piece_like = jax.ShapeDtypeStruct((rows, width), jnp.bfloat16)

    block = jax.ShapeDtypeStruct(front.shape, jnp.float32)

    def way(rnd, hops):
        pairs = []
        for g in range(n):
            half = g // (n // 2) if rnd == 0 else 1 - g // (n // 2)
            for a, b in hops:
                source, target = (a, b) if half == 1 else (n - 1 - a, n - 1 - b)
                pairs.append((g * n + source, g * n + target))
        return pairs

    def both(hop):
        return way(0, [hop]) + way(1, [hop])

    count = width // WIDTH
    here = jnp.arange(sizes.size, dtype=jnp.int32)[:, None] == lax.axis_index("gz") * count + jnp.arange(count)[None, :]
    limits = jnp.sum(jnp.where(here, sizes[:, None], 0), axis=0)
    live = (jnp.arange(WIDTH)[None, :] < limits[:, None]).reshape(1, width).astype(jnp.bfloat16)

    hops = {
        "own_a": way(0, [(0, 3), (1, 2)]),
        "own_b": way(0, [(0, 2), (1, 3)]),
        "own_c": way(0, [(2, 3), (3, 2)]),
        "far_a": way(1, [(0, 3)]),
        "far_b": way(1, [(1, 3)]),
        "far_c": way(1, [(2, 3)]),
        "near_0": way(1, [(0, 1), (3, 2)]),
        "near_1": way(1, [(1, 2)]),
        "xf_0": both((0, 1)),
        "xf_1": both((1, 2)),
        "last_0": both((2, 3)) + both((3, 2)),
        "xn_0": both((0, 1)),
        "xn_1": both((1, 2)),
    }
    y_moves = {
        "beside": (None, [(g, g ^ 1) for g in range(n)]),
        "far0": (None, [(0, 2), (3, 1)]),
        "near0": ("beside", [(0, 3), (3, 0)]),
        "far1": ("far0", [(2, 3), (1, 0)]),
        "near1": ("near0", [(3, 2), (0, 1)]),
    }
    held = {}
    sums = {}
    sent = {}
    got = {}
    pair_of_sums = jax.ShapeDtypeStruct((2, rows, rows), jnp.float32)
    packet = jax.ShapeDtypeStruct((rows + CODES, rows), jnp.int16)
    for name in plan(count_x):
        label = name.lstrip(">")
        part, _, step = label.partition("_")
        kind, d = part.rstrip("0123456789"), int("0" + part.lstrip("abcdefghijklmnopqrstuvwxyz"))
        if label in y_moves:
            source, pairs = y_moves[label]
            held[label] = lax.ppermute(panels if source is None else held[source], "gy", pairs)
        elif kind == "cross":
            held[label] = lax.ppermute(panels, "gx", [((i + d) % count_x, i) for i in range(count_x)])
        elif name[0] == ">":
            got[label] = lax.ppermute(sent[label], ("gy", "gz"), hops[f"{kind}_{step}"])
        elif label == "base":
            each = [got[f"{k}_{i}"] for k in ("own", "far") for i in "abc"] + [got["near_0"]]
            for d in range(1, count_x):
                each += [got[f"last{d}_0"], got[f"xn{d}_1"]]
            each += [sums[k] for k in ("own", "far", "near")]
            each += [sums[f"{k}{d}", "late"] for d in range(1, count_x) for k in ("xf", "xn")]
            base = call(functools.partial(base_kernel, n, count_x), [block], [front, *each], 1)
        elif label == "final":
            return call(functools.partial(final_kernel, n, count_x), [block], [base, got["near_1"]], 1)
        elif step[0] == "j":
            at = int(step[1])
            kernel = near_step_kernel if kind == "near" else crossed_step_kernel
            which = part if kind == "near" else (part, "early" if at == 1 else "late")
            before = got[f"{part}_{at - 1}"]
            sent[f"{part}_{at}"] = call(functools.partial(kernel, n), [packet], [sums[which], before], 1)
        elif kind == "last":
            sent[f"{part}_0"] = call(
                functools.partial(last_kernel, n),
                [packet],
                [sums[f"xf{d}", "late"], got[f"xf{d}_1"], sums[f"xn{d}", "late"]],
                1,
            )
        elif kind == "own":
            sums[part], held["locals"], sent["own_a"], sent["own_b"] = call(
                functools.partial(own_kernel, n),
                [pair_of_sums, jax.ShapeDtypeStruct((2, rows, width), jnp.bfloat16), packet, packet],
                [live, panels, held["beside"], panels],
                2 * square,
            )
            sent["own_c"] = sent["own_a"]
        elif kind == "far":
            sums[part], held["kept_far"], sent["far_a"] = call(
                functools.partial(far_kernel, n),
                [one_sum, piece_like, packet],
                [live, held["far0"], held["far1"], panels],
                square,
            )
            sent["far_b"] = sent["far_c"] = sent["far_a"]
        elif kind == "near":
            sums[part], sent["near_0"] = call(near_kernel, [one_sum, packet], [held["kept_near"], panels], square)
        else:
            is_early = step == "k"
            kept = "kept_far" if kind == "xf" else "kept_near"
            makes = kept not in held
            pieces = [held["near0"], held["near1"]] if makes else [held[kept]]
            packs = is_early
            done = call(
                functools.partial(crossed_kernel, kind, is_early, makes, n),
                [one_sum] + [packet] * packs + [piece_like] * makes,
                [live] * makes + [held["locals"], *pieces, held[f"cross{d}"]],
                square,
            )
            done = done if isinstance(done, (tuple, list)) else [done]
            sums[part, "early" if is_early else "late"] = done[0]
            if packs:
                sent[f"{part}_0"] = done[1]
            if makes:
                held[kept] = done[2]


def solution(mesh):
    n, count_x = mesh.shape["gz"], mesh.shape["gx"]
    in_specs = (P(("gx", "gy"), "gz"), P(), P(("gx", "gz"), "gy"))
    out_specs = P(("gx", "gz"), "gy")
    if n != 4 or mesh.shape["gy"] != n or count_x < 2:
        return jax.shard_map(plain, mesh=mesh, in_specs=in_specs, out_specs=out_specs, check_vma=False)

    def body(panels, sizes, front):
        return shards(n, count_x, panels, sizes, front)

    return jax.shard_map(body, mesh=mesh, in_specs=in_specs, out_specs=out_specs, check_vma=False)
```
